32 devices in a mesh: grp: 2 (over x), sp: 16 (over z, y, core).
Axes of the slice: x: 2, y: 2, z: 4, core: 2. Of those that a mesh axis runs over, the one named last changes fastest.
Arguments:
- field: float32 [16, 32, 1024], P('grp', 'sp'), may hold values from -6 to 6
- mix_rate: float32 [32, 1024], P('sp'), may hold values from 0.05 to 2
- react: float32 [16, 16], replicated, may hold values from -1.5 to 1.5
- particles: float32 [16, 262144], P(None, ('grp', 'sp')), may hold values from -6 to 6
- cells: int32 [2, 262144], P(None, ('grp', 'sp')), may hold values from 0 to 2047
- counts: int32 [2048], P(('grp', 'sp')), may hold values from 1 to 128
- dest: int32 [2048], P(('grp', 'sp')), may hold values from 0 to 2, as said below
Outputs:
- field_out: float32 [16, 32, 1024], P('grp', 'sp')
- spread_out: float32 [16, 32, 1024], P('grp', 'sp')
- particles_out: float32 [16, 262144], P(None, ('grp', 'sp'))
The draws below stay inside these ranges and needn't reach their ends.
Inputs may be any that keep to these rules, and one draw needn't show every extreme that they name: cells[1] refers to the slab that the slot's block reaches after migration. Among each device's 64 blocks exactly 16 have dest 1 and exactly 16 have dest 2.
All inputs are finite; a program needn't handle non-finite values.
Results may differ from the reference program's by a relative error of at most 0.0055.
Values may be sent and summed in bfloat16 or wider, within the bound.
No kernel may reach another device: no remote copies, remote signals or barrier semaphores. Data moves between devices by JAX's collectives and lax.ppermute only.
A program may use at most 64 MiB of HBM per device.

```python
import math
import jax
import jax.numpy as jnp
from jax import lax

NS = 16
LZ = 2
PLANE = 1024
ROW_LENGTH = 32
P_DEV = 8192
NB = 64
MOVE = 16
NZ = 32
P_ALL = 262144
TOTAL_BLOCKS = 2048
N_GRP = 2
N_SP = 16


def draw_dest(key, part):
    devices = TOTAL_BLOCKS // NB
    pattern = jnp.concatenate([jnp.zeros((NB - 2 * MOVE,), jnp.int32), jnp.ones((MOVE,), jnp.int32), jnp.full((MOVE,), 2, jnp.int32)])
    subkeys = jax.random.split(jax.random.fold_in(key, 7), devices)

    def shuffle(subkey):
        return jax.random.permutation(subkey, pattern)
    return jax.vmap(shuffle)(subkeys).reshape(-1)


def place_ends(values, key, least, largest):
    index_at = [jax.random.randint(jax.random.fold_in(key, axis), (), 0, length) for axis, length in enumerate(values.shape)]
    longest = values.shape.index(max(values.shape))
    beside = index_at[:longest] + [(index_at[longest] + 1) % values.shape[longest]] + index_at[longest + 1:]
    return values.at[tuple(index_at)].set(least).at[tuple(beside)].set(largest)


def level_of(own_key, shape, cuts, low, top_value):
    loudness = 1.0
    for position, parts in cuts:
        heights = jax.random.uniform(jax.random.fold_in(jax.random.fold_in(own_key, 6), position), (parts,), jnp.float32, low / len(cuts), top_value / len(cuts))
        loudness = loudness * jnp.repeat(jnp.exp(heights), shape[position] // parts).reshape((-1,) + (1,) * (len(shape) - 1 - position))
    return loudness


def noise(rng, extent, scale, most, pieces=(), kind=jnp.bfloat16):
    drawn = scale * jax.random.normal(rng, extent, jnp.float32)
    if pieces:
        drawn = drawn * level_of(rng, extent, pieces, -0.22, 0.18)
    return jnp.clip(drawn, -most, most).astype(kind)


def setup_inputs(seed: int = 0) -> dict:
    seeds = jax.random.split(jax.random.key(seed), 8)
    return {
        "field": noise(seeds[0], (NS, NZ, PLANE), 1.0, 6.0, ((0, 2), (1, 16)), jnp.float32),
        "mix_rate": jnp.clip(jnp.exp(math.log(2.0) - 3.6888794 * jax.random.uniform(seeds[1], (NZ, PLANE), jnp.float32) ** level_of(seeds[1], (NZ, PLANE), ((0, 16),), -0.2, 0.2)), 0.05, 2.0),
        "react": noise(seeds[2], (NS, NS), NS ** -0.5, 1.5, (), jnp.float32),
        "particles": noise(seeds[3], (NS, P_ALL), 1.0, 6.0, ((1, 32),), jnp.float32),
        "cells": place_ends(jax.random.randint(seeds[4], (2, P_ALL), 0, LZ * PLANE), jax.random.fold_in(seeds[4], 1), 0, (LZ * PLANE) - 1).astype(jnp.int32),
        "counts": place_ends(jax.random.randint(seeds[5], (TOTAL_BLOCKS,), 1, 129), jax.random.fold_in(seeds[5], 1), 1, 128).astype(jnp.int32),
        "dest": draw_dest(jax.random.fold_in(seeds[7], 71), 0),
    }


NU_COEF = 0.15
KAPPA = 16.0
REACT_STEP = 0.5


def diffuse_full(field):
    neighbour_slabs = jnp.roll(field, 1, axis=1) + jnp.roll(field, -1, axis=1)
    neighbour_slabs = neighbour_slabs + jnp.roll(field, 1, axis=2) + jnp.roll(field, -1, axis=2)
    neighbour_slabs = neighbour_slabs + jnp.roll(field, ROW_LENGTH, axis=2) + jnp.roll(field, -ROW_LENGTH, axis=2)
    return field + NU_COEF * (neighbour_slabs - 6.0 * field)


def live_mask(counts):
    total = counts.shape[0] * 128
    slot = jnp.arange(total, dtype=jnp.int32) % 128
    return (slot < jnp.repeat(counts, 128)).astype(jnp.float32)


def advance_all(phi, located, live, diffused, rate_flat, react):
    shared_moments = diffused.reshape(NS, -1).astype(jnp.bfloat16)
    shared_moments = lax.optimization_barrier(shared_moments)
    value = jnp.take(shared_moments, located, axis=1).astype(jnp.float32)
    weight = 1.0 - jnp.exp(-0.5 * jnp.take(rate_flat, located))
    mixed = phi + weight * (value - phi)
    stepped = mixed + REACT_STEP * jnp.tanh(jnp.dot(react.T, mixed, precision=lax.Precision.HIGHEST))
    kept = live * stepped
    rows = jnp.concatenate([kept, kept * stepped, live[None]], 0).astype(jnp.bfloat16)
    rows = lax.optimization_barrier(rows).astype(jnp.float32)
    moments = jnp.zeros((2 * NS + 1, NZ * PLANE), jnp.float32).at[:, located].add(rows)
    return stepped, moments


def relax(diffused, moments):
    flat = diffused.reshape(NS, -1)
    first = moments[:NS]
    second = moments[NS:2 * NS]
    count = moments[2 * NS]
    denom = count + KAPPA
    refreshed = flat + (first - count * flat) / denom
    spread = (second - 2.0 * flat * first + count * flat * flat) / denom
    return refreshed.reshape(NS, NZ, PLANE), spread.reshape(NS, NZ, PLANE)


def reorder_particles(values, sp_axis, blk_axis):
    keep = NB - 2 * MOVE
    stay = lax.slice_in_dim(values, 0, keep, axis=blk_axis)
    lower = lax.slice_in_dim(values, keep, keep + MOVE, axis=blk_axis)
    upper = lax.slice_in_dim(values, keep + MOVE, NB, axis=blk_axis)
    return jnp.concatenate([stay, jnp.roll(upper, 1, axis=sp_axis), jnp.roll(lower, -1, axis=sp_axis)], axis=blk_axis)


def reference(field, mix_rate, react, particles, cells, counts, dest):
    cells_dev = LZ * PLANE
    offset = jnp.tile(jnp.repeat(jnp.arange(N_SP, dtype=jnp.int32) * cells_dev, P_DEV), N_GRP)
    rate_flat = mix_rate.reshape(-1)
    live0 = live_mask(counts)
    diffused0 = diffuse_full(field)
    stepped0, moments0 = advance_all(particles, cells[0] + offset, live0, diffused0, rate_flat, react)
    refreshed, unused = relax(diffused0, moments0)
    order = jnp.argsort(dest.reshape(N_GRP, N_SP, NB), axis=-1, stable=True).astype(jnp.int32)
    blocks = stepped0.reshape(NS, N_GRP, N_SP, NB, 128)
    blocks = jnp.take_along_axis(blocks, order[None, :, :, :, None], axis=3)
    cell_blocks = jnp.take_along_axis(cells[1].reshape(N_GRP, N_SP, NB, 128), order[:, :, :, None], axis=2)
    block_counts = jnp.take_along_axis(counts.reshape(N_GRP, N_SP, NB), order, axis=2)
    moved = reorder_particles(blocks, 2, 3).reshape(NS, P_ALL)
    cell_next = reorder_particles(cell_blocks, 1, 2).reshape(P_ALL)
    count_next = reorder_particles(block_counts, 1, 2).reshape(TOTAL_BLOCKS)
    live1 = live_mask(count_next)
    diffused1 = diffuse_full(refreshed)
    stepped1, moments1 = advance_all(moved, cell_next + offset, live1, diffused1, rate_flat, react)
    field_out, spread_out = relax(diffused1, moments1)
    return field_out, spread_out, live1[None] * stepped1
```

```python
import functools
import jax
import jax.numpy as jnp
from jax import lax
from jax.experimental import pallas as pl
from jax.experimental.pallas import tpu as pltpu
from jax.sharding import PartitionSpec as P

ROW_LENGTH = 32
MOVE = 16
BLOCK = 128
LOW = 256
SPAN = 1024
SPLIT = 128.0

NU_COEF = 0.15
KAPPA = 16.0
REACT_STEP = 0.5
AXES = ("grp", "sp")
BF = jnp.bfloat16
F32 = jnp.float32


def partner(s, pairing, n_sp):
    if pairing is None:
        return s
    if pairing == 0:
        return s ^ 1
    return (((s + 1) ^ 1) - 1) % n_sp


def exchange(value, shift, pairing):
    n_grp, n_sp = lax.axis_size("grp"), lax.axis_size("sp")
    pairs = [
        (g * n_sp + s, ((g + shift) % n_grp) * n_sp + partner(s, pairing, n_sp))
        for g in range(n_grp)
        for s in range(n_sp)
    ]
    return lax.ppermute(value, AXES, pairs)


def pick(options, index):
    result = options[0]
    for position in range(1, len(options)):
        result = jnp.where(index == position, options[position], result)
    return result


def by_owner(pieces, group, n_grp):
    rows = []
    for owner in range(n_grp):
        shift = lax.rem(group - owner + n_grp, n_grp)
        rows.append(pick(pieces, shift))
    return jnp.concatenate(rows, 0) if n_grp > 1 else rows[0]


def spread_step(planes, width):
    inner = planes[width:-width]
    total = planes[2 * width :] + planes[: -2 * width]
    length = planes.shape[1]
    for amount in (1, length - 1, ROW_LENGTH, length - ROW_LENGTH):
        total = total + pltpu.roll(inner, amount, 1)
    return inner + NU_COEF * (total - 6.0 * inner)


def fill_table(table, diffused, width, parts_per_plane, depth):
    for plane in range(depth):
        for part in range(parts_per_plane):
            at = (plane * parts_per_plane + part) * width
            table[at : at + width, :] = diffused[
                plane * width : (plane + 1) * width, part * LOW : (part + 1) * LOW
            ].astype(BF)


def advance_span(phi, code, table, reaction, n_parts, squares):
    width, span = phi.shape
    column = lax.bitwise_and(code, LOW - 1)
    part = lax.shift_right_logical(code, LOW.bit_length() - 1)
    column_grid = lax.broadcasted_iota(jnp.int32, (LOW, span), 0)
    onehot = (column_grid == column).astype(F32).astype(BF)
    looked = jnp.dot(table[...], onehot, preferred_element_type=F32)
    part_rows = jnp.broadcast_to(part, (width, span))
    value = jnp.zeros((width, span), F32)
    for k in range(n_parts):
        value = jnp.where(part_rows == k, looked[k * width : (k + 1) * width], value)
    base = n_parts * width
    part_grid = lax.broadcasted_iota(jnp.int32, (n_parts, span), 0)
    mine = part_grid == part
    weights = looked[base : base + n_parts] + looked[base + n_parts : base + 2 * n_parts]
    weight = jnp.sum(jnp.where(mine, weights, 0.0), 0, keepdims=True)
    mixed = phi + weight * (value - phi)
    upper = mixed.astype(BF)
    lower = (mixed - upper.astype(F32)).astype(BF)
    drive = jnp.dot(
        reaction, jnp.concatenate([upper, lower, upper], 0), preferred_element_type=F32
    )
    stepped = mixed + REACT_STEP * jnp.tanh(drive)
    rows = [stepped, stepped * stepped] if squares else [stepped]
    deposits = []
    for row in rows:
        for k in range(n_parts):
            deposits.append(jnp.where(part_rows == k, row, 0.0).astype(BF))
    deposits.append(jnp.where(mine, 1.0, 0.0).astype(BF))
    sums = lax.dot_general(
        jnp.concatenate(deposits, 0),
        onehot,
        (((1,), (1,)), ((), ())),
        preferred_element_type=F32,
    )
    return stepped, sums


def split_count(count):
    upper = jnp.floor(count * (1.0 / SPLIT))
    return upper, count - upper * SPLIT


def reaction_rows(react):
    turned = react.T
    upper = turned.astype(BF)
    lower = (turned - upper.astype(F32)).astype(BF)
    return jnp.concatenate([upper, upper, lower], 1)


def indices():
    return lax.axis_index("grp"), lax.axis_index("sp")


def order_kernel(dest, counts, particles, cells, rate, sorted_phi, codes, weights):
    _, slab = indices()
    even = lax.rem(slab, 2) == 0
    blocks = particles.shape[1] // BLOCK
    keep = blocks - 2 * MOVE
    cells_dev = rate.shape[0] * rate.shape[1]
    lane = lax.broadcasted_iota(jnp.int32, (2, BLOCK), 1)
    stay = jnp.int32(0)
    below = jnp.where(even, keep + MOVE, keep).astype(jnp.int32)
    above = jnp.where(even, keep, keep + MOVE).astype(jnp.int32)
    for block in range(blocks):
        where = dest[block]
        place = jnp.where(where == 0, stay, jnp.where(where == 1, below, above))
        stay = stay + jnp.where(where == 0, 1, 0)
        below = below + jnp.where(where == 1, 1, 0)
        above = above + jnp.where(where == 2, 1, 0)
        at = pl.ds(pl.multiple_of(place * BLOCK, BLOCK), BLOCK)
        source = slice(block * BLOCK, (block + 1) * BLOCK)
        sorted_phi[:, at] = particles[:, source]
        codes[:, at] = jnp.where(lane < counts[block], cells[:, source], cells_dev)
    depth, plane = rate.shape
    rows = [
        rate[z : z + 1, k * LOW : (k + 1) * LOW]
        for z in range(depth)
        for k in range(plane // LOW)
    ]
    weight = 1.0 - jnp.exp(-0.5 * jnp.concatenate(rows, 0))
    upper = weight.astype(BF)
    lower = (weight - upper.astype(F32)).astype(BF)
    weights[...] = jnp.concatenate([upper, lower], 0)


def first_kernel(n_grp, own, *refs):
    n_in = 5 + 3 * n_grp
    react, sorted_phi, codes, weights, mine = refs[:5]
    fields = refs[5 : n_in - 1]
    (diffused_out, sums_out, slab_msg, pair0_msg, pair1_msg, stay_phi) = refs[n_in - 1 : n_in + 5]
    table = refs[n_in + 5]
    group, slab = indices()
    even = lax.rem(slab, 2) == 0
    width, total = sorted_phi.shape
    depth = mine.shape[0] // own
    plane = mine.shape[1]
    per_plane = plane // LOW
    n_parts = depth * per_plane
    here, low, high = [mine[...]], [], []
    position = 0
    for shift in range(n_grp):
        if shift > 0:
            here.append(fields[position][...].astype(F32))
            position += 1
        one = fields[position][...].astype(F32)
        two = fields[position + 1][...].astype(F32)
        position += 2
        low.append(jnp.where(even, two, one))
        high.append(jnp.where(even, one, two))
    planes = []
    for pieces in (low, here, high):
        for z in range(depth):
            planes.append(
                by_owner([piece[z * own : (z + 1) * own] for piece in pieces], group, n_grp)
            )
    wide = jnp.concatenate(planes[depth - 2 : 2 * depth + 2], 0)
    diffused = spread_step(wide, width)
    diffused_out[...] = diffused
    fill_table(table, diffused[width:-width], width, per_plane, depth)
    table[n_parts * width :, :] = weights[...]
    reaction = reaction_rows(react[...])
    sums_out[...] = jnp.zeros_like(sums_out)

    def body(index, carry):
        at = pl.ds(pl.multiple_of(index * SPAN, SPAN), SPAN)
        stepped, sums = advance_span(
            sorted_phi[:, at], codes[0:1, at], table, reaction, n_parts, False
        )
        stay_phi[:, at] = stepped
        sums_out[...] += sums
        return carry

    lax.fori_loop(0, total // SPAN, body, 0)
    sums = sums_out[...]
    first = sums[: n_parts * width]
    upper, lower = split_count(sums[n_parts * width :])
    digits = jnp.concatenate([upper, lower], 0).astype(BF)
    n_first = n_parts * width
    slab_msg[:n_first, :] = first.astype(BF)
    slab_msg[n_first:, :] = digits
    half = per_plane * width
    bottom = first[:half].astype(BF)
    top = first[n_first - half :].astype(BF)
    keep = total - 2 * MOVE * BLOCK
    for message, face, start in (
        (pair0_msg, jnp.where(even, top, bottom), keep),
        (pair1_msg, jnp.where(even, bottom, top), keep + MOVE * BLOCK),
    ):
        message[:half, :] = face
        message[half : half + 2 * n_parts, :] = digits
        row = half + 2 * n_parts
        pieces = MOVE * BLOCK // LOW
        columns, parts = [], []
        for k in range(pieces):
            at = slice(start + k * LOW, start + (k + 1) * LOW)
            message[row + k * width : row + (k + 1) * width, :] = stay_phi[:, at].astype(BF)
            code = codes[1:2, at]
            columns.append(lax.bitwise_and(code, LOW - 1).astype(F32))
            parts.append(lax.shift_right_logical(code, LOW.bit_length() - 1).astype(F32))
        row += pieces * width
        message[row : row + 2 * pieces, :] = jnp.concatenate(columns + parts, 0).astype(BF)


def second_kernel(n_grp, own, *refs):
    n_in = 6 + 3 * n_grp - 1
    react, stay_phi, codes, weights, diffused0, sums0 = refs[:6]
    received = refs[6:n_in]
    particles_out, own_sums, own_diffused = refs[n_in : n_in + 3]
    messages = refs[n_in + 3 : n_in + 2 + n_grp]
    table, phi, code_row, refreshed, sums = refs[n_in + 2 + n_grp :]
    group, slab = indices()
    even = lax.rem(slab, 2) == 0
    width, total = stay_phi.shape
    n_parts = weights.shape[0] // 2
    n_first = n_parts * width
    plane = diffused0.shape[1]
    per_plane = plane // LOW
    depth = n_parts // per_plane
    half = per_plane * width
    keep = total - 2 * MOVE * BLOCK
    pieces = MOVE * BLOCK // LOW

    here_first, here_count = sums0[:n_first], sums0[n_first:]
    side_first, side_count = [None, None], [None, None]
    position = 0
    moving = [None, None]
    for shift in range(n_grp):
        if shift > 0:
            slab_rows = received[position][...].astype(F32)
            position += 1
            here_first = here_first + slab_rows[:n_first]
            here_count = (
                here_count
                + slab_rows[n_first : n_first + n_parts] * SPLIT
                + slab_rows[n_first + n_parts :]
            )
        for pairing in range(2):
            message = received[position]
            position += 1
            rows = message[: half + 2 * n_parts, :].astype(F32)
            first = rows[:half]
            count = rows[half : half + n_parts] * SPLIT + rows[half + n_parts :]
            if shift == 0:
                moving[pairing] = message
                side_first[pairing], side_count[pairing] = first, count
            else:
                side_first[pairing] = side_first[pairing] + first
                side_count[pairing] = side_count[pairing] + count
    low_first = jnp.where(even, side_first[1], side_first[0])
    high_first = jnp.where(even, side_first[0], side_first[1])
    low_count = jnp.where(even, side_count[1], side_count[0])
    high_count = jnp.where(even, side_count[0], side_count[1])
    firsts = [low_first] + [here_first[z * half : (z + 1) * half] for z in range(depth)]
    firsts.append(high_first)
    counts = [low_count[n_parts - per_plane :]]
    counts += [here_count[z * per_plane : (z + 1) * per_plane] for z in range(depth)]
    counts.append(high_count[:per_plane])
    for z in range(depth + 2):
        for k in range(per_plane):
            at = slice(k * LOW, (k + 1) * LOW)
            old = diffused0[z * width : (z + 1) * width, at]
            count = counts[z][k : k + 1]
            change = firsts[z][k * width : (k + 1) * width] - count * old
            refreshed[z * width : (z + 1) * width, at] = old + change / (count + KAPPA)
    diffused = spread_step(refreshed[...], width)
    fill_table(table, diffused, width, per_plane, depth)
    table[n_first:, :] = weights[...]
    for z in range(depth):
        for k in range(per_plane):
            options = [
                diffused[z * width + j * own : z * width + (j + 1) * own, k * LOW : (k + 1) * LOW]
                for j in range(n_grp)
            ]
            at = (z * per_plane + k) * own
            own_diffused[at : at + own, :] = pick(options, group)

    phi[:, :keep] = stay_phi[:, :keep]
    code_row[:, :keep] = codes[1:2, :keep]
    starts = (
        jnp.where(even, keep + MOVE * BLOCK, keep),
        jnp.where(even, keep, keep + MOVE * BLOCK),
    )
    for pairing in range(2):
        message = moving[pairing]
        row = half + 2 * n_parts
        tail = message[row + pieces * width : row + pieces * width + 2 * pieces, :].astype(F32)
        code = (tail[:pieces] + tail[pieces:] * float(LOW)).astype(jnp.int32)
        for k in range(pieces):
            at = pl.ds(pl.multiple_of(starts[pairing] + k * LOW, LOW), LOW)
            phi[:, at] = message[row + k * width : row + (k + 1) * width, :].astype(F32)
            code_row[:, at] = code[k : k + 1]

    reaction = reaction_rows(react[...])
    sums[...] = jnp.zeros_like(sums)

    def body(index, carry):
        at = pl.ds(pl.multiple_of(index * SPAN, SPAN), SPAN)
        code = code_row[:, at]
        stepped, more = advance_span(phi[:, at], code, table, reaction, n_parts, True)
        particles_out[:, at] = jnp.where(code < n_parts * LOW, stepped, 0.0)
        sums[...] += more
        return carry

    lax.fori_loop(0, total // SPAN, body, 0)
    upper, lower = split_count(sums[2 * n_first :, :])
    digits = jnp.concatenate([upper, lower], 0).astype(BF)

    def owned(owner):
        rows = []
        for kind in range(2):
            for k in range(n_parts):
                base = kind * n_first + k * width
                rows.append(
                    pick(
                        [sums[base + j * own : base + (j + 1) * own, :] for j in range(n_grp)],
                        owner,
                    )
                )
        return jnp.concatenate(rows, 0)

    n_own = 2 * n_parts * own
    own_sums[:n_own, :] = owned(group)
    own_sums[n_own:, :] = sums[2 * n_first :, :]
    for shift in range(1, n_grp):
        message = messages[shift - 1]
        message[:n_own, :] = owned(lax.rem(group + shift, n_grp)).astype(BF)
        message[n_own:, :] = digits


def last_kernel(n_grp, own, *refs):
    own_sums, diffused = refs[:2]
    received = refs[2 : 1 + n_grp]
    field_out, spread_out = refs[1 + n_grp :]
    n_parts = diffused.shape[0] // own
    n_half = n_parts * own
    sums = own_sums[: 2 * n_half, :]
    count = own_sums[2 * n_half :, :]
    for message in received:
        rows = message[...].astype(F32)
        sums = sums + rows[: 2 * n_half]
        count = (
            count
            + rows[2 * n_half : 2 * n_half + n_parts] * SPLIT
            + rows[2 * n_half + n_parts :]
        )
    depth = field_out.shape[1]
    per_plane = n_parts // depth
    for z in range(depth):
        for k in range(per_plane):
            at = (z * per_plane + k) * own
            mean = diffused[at : at + own, :]
            first = sums[at : at + own]
            second = sums[n_half + at : n_half + at + own]
            here = count[z * per_plane + k : z * per_plane + k + 1]
            scale = 1.0 / (here + KAPPA)
            columns = slice(k * LOW, (k + 1) * LOW)
            field_out[:, z, columns] = mean + (first - here * mean) * scale
            spread_out[:, z, columns] = (
                second - 2.0 * mean * first + here * mean * mean
            ) * scale


def call(kernel, name, outs, scratch, flops, smem=0, limit=20):
    specs = [pl.BlockSpec(memory_space=pltpu.SMEM)] * smem

    def run(*args):
        return pl.pallas_call(
            kernel,
            out_shape=[jax.ShapeDtypeStruct(shape, dtype) for shape, dtype in outs],
            in_specs=specs + [pl.BlockSpec(memory_space=pltpu.VMEM)] * (len(args) - smem),
            out_specs=[pl.BlockSpec(memory_space=pltpu.VMEM)] * len(outs),
            scratch_shapes=[pltpu.VMEM(shape, dtype) for shape, dtype in scratch],
            compiler_params=pltpu.CompilerParams(vmem_limit_bytes=limit << 20),
            cost_estimate=pl.CostEstimate(flops=flops, bytes_accessed=1 << 20, transcendentals=0),
            name=name,
        )(*args)

    return run


def shards(field, mix_rate, react, particles, cells, counts, dest):
    n_grp = lax.axis_size("grp")
    own, depth, plane = field.shape
    width, total = particles.shape
    n_parts = depth * plane // LOW
    per_plane = plane // LOW
    n_first = n_parts * width
    half = per_plane * width
    pieces = MOVE * BLOCK // LOW

    mine = jnp.transpose(field, (1, 0, 2)).reshape(depth * own, plane)
    sent = mine.astype(BF)
    fields = []
    for shift in range(n_grp):
        if shift > 0:
            fields.append(exchange(sent, shift, None))
        fields.append(exchange(sent, shift, 0))
        fields.append(exchange(sent, shift, 1))
    sorted_phi, codes, weights = call(
        order_kernel,
        "order",
        [((width, total), F32), ((2, total), jnp.int32), ((2 * n_parts, LOW), BF)],
        [],
        1 << 24,
        smem=2,
        limit=8,
    )(dest, counts, particles, cells, mix_rate)

    pair_rows = half + 2 * n_parts + pieces * width + 2 * pieces
    table = ((n_first + 2 * n_parts, LOW), BF)
    diffused0, sums0, slab_msg, pair0_msg, pair1_msg, stay_phi = call(
        functools.partial(first_kernel, n_grp, own),
        "first",
        [
            (((depth + 2) * width, plane), F32),
            ((n_first + n_parts, LOW), F32),
            ((n_first + 2 * n_parts, LOW), BF),
            ((pair_rows, LOW), BF),
            ((pair_rows, LOW), BF),
            ((width, total), F32),
        ],
        [table],
        1 << 32,
    )(react, sorted_phi, codes, weights, mine, *fields)

    received = []
    faces = [message[: half + 2 * n_parts] for message in (pair0_msg, pair1_msg)]
    for shift in range(n_grp):
        if shift > 0:
            received.append(exchange(slab_msg, shift, None))
        for pairing, message in enumerate((pair0_msg, pair1_msg)):
            received.append(exchange(faces[pairing] if shift > 0 else message, shift, pairing))

    n_own = 2 * n_parts * own
    outs = call(
        functools.partial(second_kernel, n_grp, own),
        "second",
        [((width, total), F32), ((n_own + n_parts, LOW), F32), ((n_parts * own, LOW), F32)]
        + [((n_own + 2 * n_parts, LOW), BF)] * (n_grp - 1),
        [
            table,
            ((width, total), F32),
            ((1, total), jnp.int32),
            (((depth + 2) * width, plane), F32),
            ((2 * n_first + n_parts, LOW), F32),
        ],
        1 << 32,
    )(react, stay_phi, codes, weights, diffused0, sums0, *received)
    particles_out, own_sums, own_diffused = outs[:3]
    final = [exchange(outs[2 + shift], shift, None) for shift in range(1, n_grp)]
    field_out, spread_out = call(
        functools.partial(last_kernel, n_grp, own),
        "last",
        [(field.shape, F32), (field.shape, F32)],
        [],
        1 << 20,
        limit=8,
    )(own_sums, own_diffused, *final)
    return field_out, spread_out, particles_out


def solution(mesh):
    return jax.shard_map(
        shards,
        mesh=mesh,
        in_specs=(
            P("grp", "sp", None),
            P("sp", None),
            P(),
            P(None, ("grp", "sp")),
            P(None, ("grp", "sp")),
            P(("grp", "sp")),
            P(("grp", "sp")),
        ),
        out_specs=(P("grp", "sp", None), P("grp", "sp", None), P(None, ("grp", "sp"))),
        check_vma=False,
    )
```

```python
import functools
import jax
import jax.numpy as jnp
from jax import lax
from jax.experimental import pallas as pl
from jax.experimental.pallas import tpu as pltpu
from jax.sharding import PartitionSpec as P

ROW_LENGTH = 32
MOVE = 16
BLOCK = 128
LOW = 256
SPAN = 4096
UNROLL = True
STEPS = 2
SPLIT = 128.0

NU_COEF = 0.15
KAPPA = 16.0
REACT_STEP = 0.5
AXES = ("grp", "sp")
BF = jnp.bfloat16
F32 = jnp.float32


def partner(s, pairing, n_sp):
    if pairing is None:
        return s
    if pairing == 0:
        return s ^ 1
    return (((s + 1) ^ 1) - 1) % n_sp


def exchange(value, shift, pairing):
    n_grp, n_sp = lax.axis_size("grp"), lax.axis_size("sp")
    pairs = [
        (g * n_sp + s, ((g + shift) % n_grp) * n_sp + partner(s, pairing, n_sp))
        for g in range(n_grp)
        for s in range(n_sp)
    ]
    return lax.ppermute(value, AXES, pairs)


def pick(options, index):
    result = options[0]
    for position in range(1, len(options)):
        result = jnp.where(index == position, options[position], result)
    return result


def by_owner(pieces, group, n_grp):
    rows = []
    for owner in range(n_grp):
        shift = lax.rem(group - owner + n_grp, n_grp)
        rows.append(pick(pieces, shift))
    return jnp.concatenate(rows, 0) if n_grp > 1 else rows[0]


def spread_step(planes, width):
    inner = planes[width:-width]
    total = planes[2 * width :] + planes[: -2 * width]
    length = planes.shape[1]
    for amount in (1, length - 1, ROW_LENGTH, length - ROW_LENGTH):
        total = total + pltpu.roll(inner, amount, 1)
    return inner + NU_COEF * (total - 6.0 * inner)


def fill_table(table, diffused, width, parts_per_plane, depth):
    for plane in range(depth):
        for part in range(parts_per_plane):
            at = (plane * parts_per_plane + part) * width
            table[at : at + width, :] = diffused[
                plane * width : (plane + 1) * width, part * LOW : (part + 1) * LOW
            ].astype(BF)


def onehot(column):
    grid = lax.broadcasted_iota(jnp.int32, (LOW, column.shape[1]), 0).astype(F32).astype(BF)
    return jnp.where(grid == column.astype(BF), jnp.ones((), BF), jnp.zeros((), BF))


def produce(phi, code, table, reaction, n_parts):
    width, span = phi.shape
    part = lax.shift_right_logical(code, LOW.bit_length() - 1)
    column = lax.bitwise_and(code, LOW - 1).astype(F32)
    looked = jnp.dot(table[...], onehot(column), preferred_element_type=F32)
    part_rows = jnp.broadcast_to(part, (width, span))
    value = looked[:width]
    for k in range(1, n_parts):
        value = jnp.where(part_rows == k, looked[k * width : (k + 1) * width], value)
    base = n_parts * width
    mine = lax.broadcasted_iota(jnp.int32, (n_parts, span), 0) == part
    weights = looked[base : base + n_parts] + looked[base + n_parts : base + 2 * n_parts]
    weight = jnp.sum(jnp.where(mine, weights, 0.0), 0, keepdims=True)
    mixed = phi + weight * (value - phi)
    upper = mixed.astype(BF)
    lower = (mixed - upper.astype(F32)).astype(BF)
    drive = jnp.dot(
        reaction, jnp.concatenate([upper, lower, upper], 0), preferred_element_type=F32
    )
    return mixed + REACT_STEP * jnp.tanh(drive)


def consume(stepped, cell, n_parts, squares, sums):
    width, span = stepped.shape
    part = jnp.floor(cell * (1.0 / LOW))
    column = cell - part * LOW
    part_rows = jnp.broadcast_to(part.astype(BF), (width, span))
    masks = [part_rows == jnp.asarray(k, BF) for k in range(n_parts)]
    left = []
    for row in [stepped, stepped * stepped] if squares else [stepped]:
        narrow = row.astype(BF)
        left += [jnp.where(mask, narrow, jnp.zeros((), BF)) for mask in masks]
    rank = lax.broadcasted_iota(jnp.int32, (width, span), 0).astype(F32).astype(BF)
    left.append(jnp.where(rank == part_rows, jnp.ones((), BF), jnp.zeros((), BF)))
    sums[...] += lax.dot_general(
        jnp.concatenate(left, 0),
        onehot(column),
        (((1,), (1,)), ((), ())),
        preferred_element_type=F32,
    )


def advance(phi, codes, code_row, cells, table, reaction, n_parts, squares, mask_dead, out, sums):
    spans = phi.shape[1] // SPAN

    def span_at(index):
        if isinstance(index, int):
            return slice(index * SPAN, (index + 1) * SPAN)
        return pl.ds(pl.multiple_of(index * SPAN, SPAN), SPAN)

    def make(index):
        at = span_at(index)
        code = codes[code_row : code_row + 1, at]
        stepped = produce(phi[:, at], code, table, reaction, n_parts)
        out[:, at] = jnp.where(code < n_parts * LOW, stepped, 0.0) if mask_dead else stepped

    def take(index):
        at = span_at(index)
        consume(out[:, at], cells[:, at], n_parts, squares, sums)

    sums[...] = jnp.zeros_like(sums)
    make(0)
    if UNROLL:
        for index in range(1, spans):
            make(index)
            take(index - 1)
    else:

        def body(index, carry):
            for step in range(STEPS):
                make(STEPS * index + step + 1)
                take(STEPS * index + step)
            return carry

        trips = (spans - 1) // STEPS
        lax.fori_loop(0, trips, body, 0)
        for index in range(trips * STEPS + 1, spans):
            make(index)
            take(index - 1)
    take(spans - 1)


def split_count(count):
    upper = jnp.floor(count * (1.0 / SPLIT))
    return upper, count - upper * SPLIT


def reaction_rows(react):
    turned = react.T
    upper = turned.astype(BF)
    lower = (turned - upper.astype(F32)).astype(BF)
    return jnp.concatenate([upper, upper, lower], 1)


def indices():
    return lax.axis_index("grp"), lax.axis_index("sp")


def order_kernel(dest, counts, particles, cells, rate, sorted_phi, codes, cells_f, weights):
    _, slab = indices()
    even = lax.rem(slab, 2) == 0
    blocks = particles.shape[1] // BLOCK
    keep = blocks - 2 * MOVE
    cells_dev = rate.shape[0] * rate.shape[1]
    lane = lax.broadcasted_iota(jnp.int32, (2, BLOCK), 1)
    stay = jnp.int32(0)
    below = jnp.where(even, keep + MOVE, keep).astype(jnp.int32)
    above = jnp.where(even, keep, keep + MOVE).astype(jnp.int32)
    for block in range(blocks):
        where = dest[block]
        place = jnp.where(where == 0, stay, jnp.where(where == 1, below, above))
        stay = stay + jnp.where(where == 0, 1, 0)
        below = below + jnp.where(where == 1, 1, 0)
        above = above + jnp.where(where == 2, 1, 0)
        at = pl.ds(pl.multiple_of(place * BLOCK, BLOCK), BLOCK)
        source = slice(block * BLOCK, (block + 1) * BLOCK)
        sorted_phi[:, at] = particles[:, source]
        code = jnp.where(lane < counts[block], cells[:, source], cells_dev)
        codes[:, at] = code
        cells_f[:, at] = code[0:1].astype(F32)
    depth, plane = rate.shape
    rows = [
        rate[z : z + 1, k * LOW : (k + 1) * LOW]
        for z in range(depth)
        for k in range(plane // LOW)
    ]
    weight = 1.0 - jnp.exp(-0.5 * jnp.concatenate(rows, 0))
    upper = weight.astype(BF)
    lower = (weight - upper.astype(F32)).astype(BF)
    weights[...] = jnp.concatenate([upper, lower], 0)


def first_kernel(n_grp, own, *refs):
    n_in = 6 + 3 * n_grp
    react, sorted_phi, codes, cells_f, weights, mine = refs[:6]
    fields = refs[6 : n_in - 1]
    (diffused_out, sums_out, slab_msg, pair0_msg, pair1_msg, stay_phi) = refs[n_in - 1 : n_in + 5]
    table, sums_all = refs[n_in + 5 : n_in + 7]
    group, slab = indices()
    even = lax.rem(slab, 2) == 0
    width, total = sorted_phi.shape
    depth = mine.shape[0] // own
    plane = mine.shape[1]
    per_plane = plane // LOW
    n_parts = depth * per_plane
    here, low, high = [mine[...]], [], []
    position = 0
    for shift in range(n_grp):
        if shift > 0:
            here.append(fields[position][...].astype(F32))
            position += 1
        one = fields[position][...].astype(F32)
        two = fields[position + 1][...].astype(F32)
        position += 2
        low.append(jnp.where(even, two, one))
        high.append(jnp.where(even, one, two))
    planes = []
    for pieces in (low, here, high):
        for z in range(depth):
            planes.append(
                by_owner([piece[z * own : (z + 1) * own] for piece in pieces], group, n_grp)
            )
    wide = jnp.concatenate(planes[depth - 2 : 2 * depth + 2], 0)
    diffused = spread_step(wide, width)
    diffused_out[...] = diffused
    fill_table(table, diffused[width:-width], width, per_plane, depth)
    table[n_parts * width :, :] = weights[...]
    reaction = reaction_rows(react[...])
    advance(
        sorted_phi, codes, 0, cells_f, table, reaction, n_parts, False, False, stay_phi, sums_all
    )
    sums_out[...] = sums_all[: (width + 1) * n_parts, :]
    sums = sums_out[...]
    first = sums[: n_parts * width]
    upper, lower = split_count(sums[n_parts * width :])
    digits = jnp.concatenate([upper, lower], 0).astype(BF)
    n_first = n_parts * width
    slab_msg[:n_first, :] = first.astype(BF)
    slab_msg[n_first:, :] = digits
    half = per_plane * width
    bottom = first[:half].astype(BF)
    top = first[n_first - half :].astype(BF)
    keep = total - 2 * MOVE * BLOCK
    for message, face, start in (
        (pair0_msg, jnp.where(even, top, bottom), keep),
        (pair1_msg, jnp.where(even, bottom, top), keep + MOVE * BLOCK),
    ):
        message[:half, :] = face
        message[half : half + 2 * n_parts, :] = digits
        row = half + 2 * n_parts
        pieces = MOVE * BLOCK // LOW
        tails, parts = [], []
        for k in range(pieces):
            at = slice(start + k * LOW, start + (k + 1) * LOW)
            message[row + k * width : row + (k + 1) * width, :] = stay_phi[:, at].astype(BF)
            code = codes[1:2, at]
            tails.append(lax.bitwise_and(code, LOW - 1).astype(F32))
            parts.append(lax.shift_right_logical(code, LOW.bit_length() - 1).astype(F32))
        row += pieces * width
        message[row : row + 2 * pieces, :] = jnp.concatenate(tails + parts, 0).astype(BF)


def second_kernel(n_grp, own, *refs):
    n_in = 6 + 3 * n_grp - 1
    react, stay_phi, codes, weights, diffused0, sums0 = refs[:6]
    received = refs[6:n_in]
    particles_out, own_sums, own_diffused = refs[n_in : n_in + 3]
    messages = refs[n_in + 3 : n_in + 2 + n_grp]
    table, phi, code_row, cells_f, refreshed, sums = refs[n_in + 2 + n_grp :]
    group, slab = indices()
    even = lax.rem(slab, 2) == 0
    width, total = stay_phi.shape
    n_parts = weights.shape[0] // 2
    n_first = n_parts * width
    plane = diffused0.shape[1]
    per_plane = plane // LOW
    depth = n_parts // per_plane
    half = per_plane * width
    keep = total - 2 * MOVE * BLOCK
    pieces = MOVE * BLOCK // LOW

    here_first, here_count = sums0[:n_first], sums0[n_first:]
    side_first, side_count = [None, None], [None, None]
    position = 0
    moving = [None, None]
    for shift in range(n_grp):
        if shift > 0:
            slab_rows = received[position][...].astype(F32)
            position += 1
            here_first = here_first + slab_rows[:n_first]
            here_count = (
                here_count
                + slab_rows[n_first : n_first + n_parts] * SPLIT
                + slab_rows[n_first + n_parts :]
            )
        for pairing in range(2):
            message = received[position]
            position += 1
            rows = message[: half + 2 * n_parts, :].astype(F32)
            first = rows[:half]
            count = rows[half : half + n_parts] * SPLIT + rows[half + n_parts :]
            if shift == 0:
                moving[pairing] = message
                side_first[pairing], side_count[pairing] = first, count
            else:
                side_first[pairing] = side_first[pairing] + first
                side_count[pairing] = side_count[pairing] + count
    low_first = jnp.where(even, side_first[1], side_first[0])
    high_first = jnp.where(even, side_first[0], side_first[1])
    low_count = jnp.where(even, side_count[1], side_count[0])
    high_count = jnp.where(even, side_count[0], side_count[1])
    firsts = [low_first] + [here_first[z * half : (z + 1) * half] for z in range(depth)]
    firsts.append(high_first)
    counts = [low_count[n_parts - per_plane :]]
    counts += [here_count[z * per_plane : (z + 1) * per_plane] for z in range(depth)]
    counts.append(high_count[:per_plane])
    for z in range(depth + 2):
        for k in range(per_plane):
            at = slice(k * LOW, (k + 1) * LOW)
            old = diffused0[z * width : (z + 1) * width, at]
            count = counts[z][k : k + 1]
            change = firsts[z][k * width : (k + 1) * width] - count * old
            refreshed[z * width : (z + 1) * width, at] = old + change / (count + KAPPA)
    diffused = spread_step(refreshed[...], width)
    fill_table(table, diffused, width, per_plane, depth)
    table[n_first:, :] = weights[...]
    for z in range(depth):
        for k in range(per_plane):
            options = [
                diffused[z * width + j * own : z * width + (j + 1) * own, k * LOW : (k + 1) * LOW]
                for j in range(n_grp)
            ]
            at = (z * per_plane + k) * own
            own_diffused[at : at + own, :] = pick(options, group)

    phi[:, :keep] = stay_phi[:, :keep]
    code_row[:, :keep] = codes[1:2, :keep]
    cells_f[:, :keep] = codes[1:2, :keep].astype(F32)
    starts = (
        jnp.where(even, keep + MOVE * BLOCK, keep),
        jnp.where(even, keep, keep + MOVE * BLOCK),
    )
    for pairing in range(2):
        message = moving[pairing]
        row = half + 2 * n_parts
        tail = message[row + pieces * width : row + pieces * width + 2 * pieces, :].astype(F32)
        cell = tail[:pieces] + tail[pieces:] * float(LOW)
        code = cell.astype(jnp.int32)
        for k in range(pieces):
            at = pl.ds(pl.multiple_of(starts[pairing] + k * LOW, LOW), LOW)
            phi[:, at] = message[row + k * width : row + (k + 1) * width, :].astype(F32)
            code_row[:, at] = code[k : k + 1]
            cells_f[:, at] = cell[k : k + 1]

    reaction = reaction_rows(react[...])
    advance(
        phi, code_row, 0, cells_f, table, reaction, n_parts, True, True, particles_out, sums
    )
    upper, lower = split_count(sums[2 * n_first : 2 * n_first + n_parts, :])
    digits = jnp.concatenate([upper, lower], 0).astype(BF)

    def owned(owner):
        rows = []
        for kind in range(2):
            for k in range(n_parts):
                base = kind * n_first + k * width
                rows.append(
                    pick(
                        [sums[base + j * own : base + (j + 1) * own, :] for j in range(n_grp)],
                        owner,
                    )
                )
        return jnp.concatenate(rows, 0)

    n_own = 2 * n_parts * own
    own_sums[:n_own, :] = owned(group)
    own_sums[n_own:, :] = sums[2 * n_first : 2 * n_first + n_parts, :]
    for shift in range(1, n_grp):
        message = messages[shift - 1]
        message[:n_own, :] = owned(lax.rem(group + shift, n_grp)).astype(BF)
        message[n_own:, :] = digits


def last_kernel(n_grp, own, *refs):
    own_sums, diffused = refs[:2]
    received = refs[2 : 1 + n_grp]
    field_out, spread_out = refs[1 + n_grp :]
    n_parts = diffused.shape[0] // own
    n_half = n_parts * own
    sums = own_sums[: 2 * n_half, :]
    count = own_sums[2 * n_half :, :]
    for message in received:
        rows = message[...].astype(F32)
        sums = sums + rows[: 2 * n_half]
        count = (
            count
            + rows[2 * n_half : 2 * n_half + n_parts] * SPLIT
            + rows[2 * n_half + n_parts :]
        )
    depth = field_out.shape[1]
    per_plane = n_parts // depth
    for z in range(depth):
        for k in range(per_plane):
            at = (z * per_plane + k) * own
            mean = diffused[at : at + own, :]
            first = sums[at : at + own]
            second = sums[n_half + at : n_half + at + own]
            here = count[z * per_plane + k : z * per_plane + k + 1]
            scale = 1.0 / (here + KAPPA)
            cells_f = slice(k * LOW, (k + 1) * LOW)
            field_out[:, z, cells_f] = mean + (first - here * mean) * scale
            spread_out[:, z, cells_f] = (
                second - 2.0 * mean * first + here * mean * mean
            ) * scale


def call(kernel, name, outs, scratch, flops, smem=0, limit=20):
    specs = [pl.BlockSpec(memory_space=pltpu.SMEM)] * smem

    def run(*args):
        return pl.pallas_call(
            kernel,
            out_shape=[jax.ShapeDtypeStruct(shape, dtype) for shape, dtype in outs],
            in_specs=specs + [pl.BlockSpec(memory_space=pltpu.VMEM)] * (len(args) - smem),
            out_specs=[pl.BlockSpec(memory_space=pltpu.VMEM)] * len(outs),
            scratch_shapes=[pltpu.VMEM(shape, dtype) for shape, dtype in scratch],
            compiler_params=pltpu.CompilerParams(vmem_limit_bytes=limit << 20),
            cost_estimate=pl.CostEstimate(flops=flops, bytes_accessed=1 << 20, transcendentals=0),
            name=name,
        )(*args)

    return run


def shards(field, mix_rate, react, particles, cells, counts, dest):
    n_grp = lax.axis_size("grp")
    own, depth, plane = field.shape
    width, total = particles.shape
    n_parts = depth * plane // LOW
    per_plane = plane // LOW
    n_first = n_parts * width
    half = per_plane * width
    pieces = MOVE * BLOCK // LOW

    mine = jnp.transpose(field, (1, 0, 2)).reshape(depth * own, plane)
    sent = mine.astype(BF)
    fields = []
    for shift in range(n_grp):
        if shift > 0:
            fields.append(exchange(sent, shift, None))
        fields.append(exchange(sent, shift, 0))
        fields.append(exchange(sent, shift, 1))
    sorted_phi, codes, cells_f, weights = call(
        order_kernel,
        "order",
        [
            ((width, total), F32),
            ((2, total), jnp.int32),
            ((1, total), F32),
            ((2 * n_parts, LOW), BF),
        ],
        [],
        1 << 24,
        smem=2,
        limit=8,
    )(dest, counts, particles, cells, mix_rate)

    pair_rows = half + 2 * n_parts + pieces * width + 2 * pieces
    table = ((n_first + 2 * n_parts, LOW), BF)
    diffused0, sums0, slab_msg, pair0_msg, pair1_msg, stay_phi = call(
        functools.partial(first_kernel, n_grp, own),
        "first",
        [
            (((depth + 2) * width, plane), F32),
            ((n_first + n_parts, LOW), F32),
            ((n_first + 2 * n_parts, LOW), BF),
            ((pair_rows, LOW), BF),
            ((pair_rows, LOW), BF),
            ((width, total), F32),
        ],
        [table, ((n_first + width, LOW), F32)],
        1 << 32,
    )(react, sorted_phi, codes, cells_f, weights, mine, *fields)

    received = []
    faces = [message[: half + 2 * n_parts] for message in (pair0_msg, pair1_msg)]
    for shift in range(n_grp):
        if shift > 0:
            received.append(exchange(slab_msg, shift, None))
        for pairing, message in enumerate((pair0_msg, pair1_msg)):
            received.append(exchange(faces[pairing] if shift > 0 else message, shift, pairing))

    n_own = 2 * n_parts * own
    outs = call(
        functools.partial(second_kernel, n_grp, own),
        "second",
        [((width, total), F32), ((n_own + n_parts, LOW), F32), ((n_parts * own, LOW), F32)]
        + [((n_own + 2 * n_parts, LOW), BF)] * (n_grp - 1),
        [
            table,
            ((width, total), F32),
            ((1, total), jnp.int32),
            ((1, total), F32),
            (((depth + 2) * width, plane), F32),
            ((2 * n_first + width, LOW), F32),
        ],
        1 << 32,
    )(react, stay_phi, codes, weights, diffused0, sums0, *received)
    particles_out, own_sums, own_diffused = outs[:3]
    final = [exchange(outs[2 + shift], shift, None) for shift in range(1, n_grp)]
    field_out, spread_out = call(
        functools.partial(last_kernel, n_grp, own),
        "last",
        [(field.shape, F32), (field.shape, F32)],
        [],
        1 << 20,
        limit=8,
    )(own_sums, own_diffused, *final)
    return field_out, spread_out, particles_out


def solution(mesh):
    return jax.shard_map(
        shards,
        mesh=mesh,
        in_specs=(
            P("grp", "sp", None),
            P("sp", None),
            P(),
            P(None, ("grp", "sp")),
            P(None, ("grp", "sp")),
            P(("grp", "sp")),
            P(("grp", "sp")),
        ),
        out_specs=(P("grp", "sp", None), P("grp", "sp", None), P(None, ("grp", "sp"))),
        check_vma=False,
    )
```

```python
import functools
import jax
import jax.numpy as jnp
from jax import lax
from jax.experimental import pallas as pl
from jax.experimental.pallas import tpu as pltpu
from jax.sharding import PartitionSpec as P


ROW_LENGTH = 32
MOVE = 16
BLOCK = 128
LOW = 256
SPAN = 8192
SPLIT = 128.0

NU_COEF = 0.15
KAPPA = 16.0
REACT_STEP = 0.5
AXES = ("grp", "sp")
BF = jnp.bfloat16
F32 = jnp.float32


def partner(s, pairing, n_sp):
    if pairing is None:
        return s
    if pairing == 0:
        return s ^ 1
    return (((s + 1) ^ 1) - 1) % n_sp


def exchange(value, kind, shift):
    n_grp, n_sp = lax.axis_size("grp"), lax.axis_size("sp")
    pairing = {"near": 0, "relay": 0, "far": 1, "same": None}[kind]
    step = 0 if kind == "relay" else shift
    pairs = [
        (g * n_sp + s, ((g + step) % n_grp) * n_sp + partner(s, pairing, n_sp))
        for g in range(n_grp)
        for s in range(n_sp)
    ]
    return lax.ppermute(value, AXES, pairs)


def pick(options, index):
    result = options[0]
    for position in range(1, len(options)):
        result = jnp.where(index == position, options[position], result)
    return result


def by_owner(pieces, group, n_grp):
    rows = []
    for owner in range(n_grp):
        shift = lax.rem(group - owner + n_grp, n_grp)
        rows.append(pick(pieces, shift))
    return jnp.concatenate(rows, 0) if n_grp > 1 else rows[0]


def spread_step(planes, width):
    inner = planes[width:-width]
    total = planes[2 * width :] + planes[: -2 * width]
    length = planes.shape[1]
    for amount in (1, length - 1, ROW_LENGTH, length - ROW_LENGTH):
        total = total + pltpu.roll(inner, amount, 1)
    return inner + NU_COEF * (total - 6.0 * inner)


def fill_table(table, diffused, width, parts_per_plane, depth):
    for plane in range(depth):
        for part in range(parts_per_plane):
            at = (plane * parts_per_plane + part) * width
            table[at : at + width, :] = diffused[
                plane * width : (plane + 1) * width, part * LOW : (part + 1) * LOW
            ].astype(BF)


def onehot(column):
    grid = lax.broadcasted_iota(jnp.int32, (LOW, column.shape[1]), 0).astype(F32).astype(BF)
    return jnp.where(grid == column.astype(BF), jnp.ones((), BF), jnp.zeros((), BF))


def produce(phi, code, table, reaction, n_parts):
    width, span = phi.shape
    part = lax.shift_right_logical(code, LOW.bit_length() - 1)
    column = lax.bitwise_and(code, LOW - 1).astype(F32)
    looked = jnp.dot(table[...], onehot(column), preferred_element_type=F32)
    part_rows = jnp.broadcast_to(part, (width, span))
    value = looked[:width]
    for k in range(1, n_parts):
        value = jnp.where(part_rows == k, looked[k * width : (k + 1) * width], value)
    base = n_parts * width
    mine = lax.broadcasted_iota(jnp.int32, (n_parts, span), 0) == part
    weights = looked[base : base + n_parts] + looked[base + n_parts : base + 2 * n_parts]
    weight = jnp.sum(jnp.where(mine, weights, 0.0), 0, keepdims=True)
    mixed = phi + weight * (value - phi)
    upper = mixed.astype(BF)
    lower = (mixed - upper.astype(F32)).astype(BF)
    drive = jnp.dot(
        reaction, jnp.concatenate([upper, lower, upper], 0), preferred_element_type=F32
    )
    return mixed + REACT_STEP * jnp.tanh(drive)


def consume(stepped, cell, n_parts, squares, sums):
    width, span = stepped.shape
    part = jnp.floor(cell * (1.0 / LOW))
    column = cell - part * LOW
    part_rows = jnp.broadcast_to(part.astype(BF), (width, span))
    masks = [part_rows == jnp.asarray(k, BF) for k in range(n_parts)]
    left = []
    for row in [stepped, stepped * stepped] if squares else [stepped]:
        narrow = row.astype(BF)
        left += [jnp.where(mask, narrow, jnp.zeros((), BF)) for mask in masks]
    rank = lax.broadcasted_iota(jnp.int32, (width, span), 0).astype(F32).astype(BF)
    left.append(jnp.where(rank == part_rows, jnp.ones((), BF), jnp.zeros((), BF)))
    sums[...] += lax.dot_general(
        jnp.concatenate(left, 0),
        onehot(column),
        (((1,), (1,)), ((), ())),
        preferred_element_type=F32,
    )


def advance(phi, codes, code_row, cells, table, reaction, n_parts, squares, mask_dead, out, sums):
    span = min(SPAN, phi.shape[1])
    spans = phi.shape[1] // span

    def span_at(index):
        return slice(index * span, (index + 1) * span)

    def make(index):
        at = span_at(index)
        code = codes[code_row : code_row + 1, at]
        stepped = produce(phi[:, at], code, table, reaction, n_parts)
        out[:, at] = jnp.where(code < n_parts * LOW, stepped, 0.0) if mask_dead else stepped

    def take(index):
        at = span_at(index)
        consume(out[:, at], cells[:, at], n_parts, squares, sums)

    sums[...] = jnp.zeros_like(sums)
    make(0)
    for index in range(1, spans):
        make(index)
        take(index - 1)
    take(spans - 1)


def split_count(count):
    upper = jnp.floor(count * (1.0 / SPLIT))
    return upper, count - upper * SPLIT


def reaction_rows(react):
    turned = react.T
    upper = turned.astype(BF)
    lower = (turned - upper.astype(F32)).astype(BF)
    return jnp.concatenate([upper, upper, lower], 1)


def indices():
    return lax.axis_index("grp"), lax.axis_index("sp")


def order_kernel(dest, counts, particles, cells, rate, sorted_phi, codes, cells_f, weights):
    _, slab = indices()
    even = lax.rem(slab, 2) == 0
    blocks = particles.shape[1] // BLOCK
    keep = blocks - 2 * MOVE
    cells_dev = rate.shape[0] * rate.shape[1]
    lane = lax.broadcasted_iota(jnp.int32, (2, BLOCK), 1)
    stay = jnp.int32(0)
    below = jnp.where(even, keep + MOVE, keep).astype(jnp.int32)
    above = jnp.where(even, keep, keep + MOVE).astype(jnp.int32)
    for block in range(blocks):
        where = dest[block]
        place = jnp.where(where == 0, stay, jnp.where(where == 1, below, above))
        stay = stay + jnp.where(where == 0, 1, 0)
        below = below + jnp.where(where == 1, 1, 0)
        above = above + jnp.where(where == 2, 1, 0)
        at = pl.ds(pl.multiple_of(place * BLOCK, BLOCK), BLOCK)
        source = slice(block * BLOCK, (block + 1) * BLOCK)
        sorted_phi[:, at] = particles[:, source]
        code = jnp.where(lane < counts[block], cells[:, source], cells_dev)
        codes[:, at] = code
        cells_f[:, at] = code[0:1].astype(F32)
    depth, plane = rate.shape
    rows = [
        rate[z : z + 1, k * LOW : (k + 1) * LOW]
        for z in range(depth)
        for k in range(plane // LOW)
    ]
    weight = 1.0 - jnp.exp(-0.5 * jnp.concatenate(rows, 0))
    upper = weight.astype(BF)
    lower = (weight - upper.astype(F32)).astype(BF)
    weights[...] = jnp.concatenate([upper, lower], 0)


def first_kernel(n_grp, own, *refs):
    n_in = 6 + 3 * n_grp
    react, sorted_phi, codes, cells_f, weights, mine = refs[:6]
    fields = refs[6 : n_in - 1]
    (diffused_out, sums_out, slab_msg, pair0_msg, pair1_msg, stay_phi) = refs[n_in - 1 : n_in + 5]
    table, sums_all = refs[n_in + 5 : n_in + 7]
    group, slab = indices()
    even = lax.rem(slab, 2) == 0
    width, total = sorted_phi.shape
    depth = mine.shape[0] // own
    plane = mine.shape[1]
    per_plane = plane // LOW
    n_parts = depth * per_plane
    here, low, high = [mine[...]], [], []
    position = 0
    for shift in range(n_grp):
        if shift > 0:
            here.append(fields[position][...].astype(F32))
            position += 1
        one = fields[position][...].astype(F32)
        two = fields[position + 1][...].astype(F32)
        position += 2
        low.append(jnp.where(even, two, one))
        high.append(jnp.where(even, one, two))
    planes = []
    for pieces in (low, here, high):
        for z in range(depth):
            planes.append(
                by_owner([piece[z * own : (z + 1) * own] for piece in pieces], group, n_grp)
            )
    wide = jnp.concatenate(planes[depth - 2 : 2 * depth + 2], 0)
    diffused = spread_step(wide, width)
    diffused_out[...] = diffused
    fill_table(table, diffused[width:-width], width, per_plane, depth)
    table[n_parts * width :, :] = weights[...]
    reaction = reaction_rows(react[...])
    advance(
        sorted_phi, codes, 0, cells_f, table, reaction, n_parts, False, False, stay_phi, sums_all
    )
    sums_out[...] = sums_all[: (width + 1) * n_parts, :]
    sums = sums_out[...]
    first = sums[: n_parts * width]
    upper, lower = split_count(sums[n_parts * width :])
    digits = jnp.concatenate([upper, lower], 0).astype(BF)
    n_first = n_parts * width
    slab_msg[:n_first, :] = first.astype(BF)
    slab_msg[n_first:, :] = digits
    half = per_plane * width
    bottom = first[:half].astype(BF)
    top = first[n_first - half :].astype(BF)
    keep = total - 2 * MOVE * BLOCK
    for message, face, start in (
        (pair0_msg, jnp.where(even, top, bottom), keep),
        (pair1_msg, jnp.where(even, bottom, top), keep + MOVE * BLOCK),
    ):
        message[:half, :] = face
        message[half : half + 2 * n_parts, :] = digits
        row = half + 2 * n_parts
        pieces = MOVE * BLOCK // LOW
        tails, parts = [], []
        for k in range(pieces):
            at = slice(start + k * LOW, start + (k + 1) * LOW)
            message[row + k * width : row + (k + 1) * width, :] = stay_phi[:, at].astype(BF)
            code = codes[1:2, at]
            tails.append(lax.bitwise_and(code, LOW - 1).astype(F32))
            parts.append(lax.shift_right_logical(code, LOW.bit_length() - 1).astype(F32))
        row += pieces * width
        message[row : row + 2 * pieces, :] = jnp.concatenate(tails + parts, 0).astype(BF)


def second_kernel(n_grp, own, *refs):
    n_in = 6 + 3 * n_grp - 1
    react, stay_phi, codes, weights, diffused0, sums0 = refs[:6]
    received = refs[6:n_in]
    particles_out, own_sums, own_diffused = refs[n_in : n_in + 3]
    messages = refs[n_in + 3 : n_in + 2 + n_grp]
    table, phi, code_row, cells_f, refreshed, sums = refs[n_in + 2 + n_grp :]
    group, slab = indices()
    even = lax.rem(slab, 2) == 0
    width, total = stay_phi.shape
    n_parts = weights.shape[0] // 2
    n_first = n_parts * width
    plane = diffused0.shape[1]
    per_plane = plane // LOW
    depth = n_parts // per_plane
    half = per_plane * width
    keep = total - 2 * MOVE * BLOCK
    pieces = MOVE * BLOCK // LOW

    here_first, here_count = sums0[:n_first], sums0[n_first:]
    side_first, side_count = [None, None], [None, None]
    position = 0
    moving = [None, None]
    for shift in range(n_grp):
        if shift > 0:
            slab_rows = received[position][...].astype(F32)
            position += 1
            here_first = here_first + slab_rows[:n_first]
            here_count = (
                here_count
                + slab_rows[n_first : n_first + n_parts] * SPLIT
                + slab_rows[n_first + n_parts :]
            )
        for pairing in range(2):
            message = received[position]
            position += 1
            if shift == 0:
                moving[pairing] = message
            if shift > 0 and pairing == 0:
                rows = message[...].astype(F32)
                first = jnp.where(even, rows[:half], rows[n_first - half : n_first])
                rows = rows[n_first:]
            else:
                rows = message[: half + 2 * n_parts, :].astype(F32)
                first = rows[:half]
                rows = rows[half:]
            count = rows[:n_parts] * SPLIT + rows[n_parts:]
            if shift == 0:
                side_first[pairing], side_count[pairing] = first, count
            else:
                side_first[pairing] = side_first[pairing] + first
                side_count[pairing] = side_count[pairing] + count
    low_first = jnp.where(even, side_first[1], side_first[0])
    high_first = jnp.where(even, side_first[0], side_first[1])
    low_count = jnp.where(even, side_count[1], side_count[0])
    high_count = jnp.where(even, side_count[0], side_count[1])
    firsts = [low_first] + [here_first[z * half : (z + 1) * half] for z in range(depth)]
    firsts.append(high_first)
    counts = [low_count[n_parts - per_plane :]]
    counts += [here_count[z * per_plane : (z + 1) * per_plane] for z in range(depth)]
    counts.append(high_count[:per_plane])
    for z in range(depth + 2):
        for k in range(per_plane):
            at = slice(k * LOW, (k + 1) * LOW)
            old = diffused0[z * width : (z + 1) * width, at]
            count = counts[z][k : k + 1]
            change = firsts[z][k * width : (k + 1) * width] - count * old
            refreshed[z * width : (z + 1) * width, at] = old + change / (count + KAPPA)
    diffused = spread_step(refreshed[...], width)
    fill_table(table, diffused, width, per_plane, depth)
    table[n_first:, :] = weights[...]
    for z in range(depth):
        for k in range(per_plane):
            options = [
                diffused[z * width + j * own : z * width + (j + 1) * own, k * LOW : (k + 1) * LOW]
                for j in range(n_grp)
            ]
            at = (z * per_plane + k) * own
            own_diffused[at : at + own, :] = pick(options, group)

    phi[:, :keep] = stay_phi[:, :keep]
    code_row[:, :keep] = codes[1:2, :keep]
    cells_f[:, :keep] = codes[1:2, :keep].astype(F32)
    starts = (
        jnp.where(even, keep + MOVE * BLOCK, keep),
        jnp.where(even, keep, keep + MOVE * BLOCK),
    )
    for pairing in range(2):
        message = moving[pairing]
        row = half + 2 * n_parts
        tail = message[row + pieces * width : row + pieces * width + 2 * pieces, :].astype(F32)
        cell = tail[:pieces] + tail[pieces:] * float(LOW)
        code = cell.astype(jnp.int32)
        for k in range(pieces):
            at = pl.ds(pl.multiple_of(starts[pairing] + k * LOW, LOW), LOW)
            phi[:, at] = message[row + k * width : row + (k + 1) * width, :].astype(F32)
            code_row[:, at] = code[k : k + 1]
            cells_f[:, at] = cell[k : k + 1]

    reaction = reaction_rows(react[...])
    advance(
        phi, code_row, 0, cells_f, table, reaction, n_parts, True, True, particles_out, sums
    )
    upper, lower = split_count(sums[2 * n_first : 2 * n_first + n_parts, :])
    digits = jnp.concatenate([upper, lower], 0).astype(BF)

    def owned(owner):
        rows = []
        for kind in range(2):
            for k in range(n_parts):
                base = kind * n_first + k * width
                rows.append(
                    pick(
                        [sums[base + j * own : base + (j + 1) * own, :] for j in range(n_grp)],
                        owner,
                    )
                )
        return jnp.concatenate(rows, 0)

    n_own = 2 * n_parts * own
    own_sums[:n_own, :] = owned(group)
    own_sums[n_own:, :] = sums[2 * n_first : 2 * n_first + n_parts, :]
    for shift in range(1, n_grp):
        message = messages[shift - 1]
        message[:n_own, :] = owned(lax.rem(group + shift, n_grp)).astype(BF)
        message[n_own:, :] = digits


def last_kernel(n_grp, own, *refs):
    own_sums, diffused = refs[:2]
    received = refs[2 : 1 + n_grp]
    field_out, spread_out = refs[1 + n_grp :]
    n_parts = diffused.shape[0] // own
    n_half = n_parts * own
    sums = own_sums[: 2 * n_half, :]
    count = own_sums[2 * n_half :, :]
    for message in received:
        rows = message[...].astype(F32)
        sums = sums + rows[: 2 * n_half]
        count = (
            count
            + rows[2 * n_half : 2 * n_half + n_parts] * SPLIT
            + rows[2 * n_half + n_parts :]
        )
    depth = field_out.shape[1]
    per_plane = n_parts // depth
    for z in range(depth):
        for k in range(per_plane):
            at = (z * per_plane + k) * own
            mean = diffused[at : at + own, :]
            first = sums[at : at + own]
            second = sums[n_half + at : n_half + at + own]
            here = count[z * per_plane + k : z * per_plane + k + 1]
            scale = 1.0 / (here + KAPPA)
            cells_f = slice(k * LOW, (k + 1) * LOW)
            field_out[:, z, cells_f] = mean + (first - here * mean) * scale
            spread_out[:, z, cells_f] = (
                second - 2.0 * mean * first + here * mean * mean
            ) * scale


def call(kernel, outs, scratch, flops, smem=0, limit=20):
    specs = [pl.BlockSpec(memory_space=pltpu.SMEM)] * smem

    def run(*args):
        return pl.pallas_call(
            kernel,
            out_shape=[jax.ShapeDtypeStruct(shape, dtype) for shape, dtype in outs],
            in_specs=specs + [pl.BlockSpec(memory_space=pltpu.VMEM)] * (len(args) - smem),
            out_specs=[pl.BlockSpec(memory_space=pltpu.VMEM)] * len(outs),
            scratch_shapes=[pltpu.VMEM(shape, dtype) for shape, dtype in scratch],
            compiler_params=pltpu.CompilerParams(vmem_limit_bytes=limit << 20),
            cost_estimate=pl.CostEstimate(flops=flops, bytes_accessed=1 << 20, transcendentals=0),
        )(*args)

    return run


def shards(field, mix_rate, react, particles, cells, counts, dest):
    n_grp = lax.axis_size("grp")
    own, depth, plane = field.shape
    width, total = particles.shape
    n_parts = depth * plane // LOW
    per_plane = plane // LOW
    n_first = n_parts * width
    half = per_plane * width
    pieces = MOVE * BLOCK // LOW

    mine = jnp.transpose(field, (1, 0, 2)).reshape(depth * own, plane)
    sent = mine.astype(BF)
    fields = []
    for shift in range(n_grp):
        near = exchange(sent, "near", shift)
        if shift > 0:
            fields.append(exchange(near, "relay", shift))
        fields += [near, exchange(sent, "far", shift)]
    sorted_phi, codes, cells_f, weights = call(
        order_kernel,
        [
            ((width, total), F32),
            ((2, total), jnp.int32),
            ((1, total), F32),
            ((2 * n_parts, LOW), BF),
        ],
        [],
        1 << 24,
        smem=2,
        limit=8,
    )(dest, counts, particles, cells, mix_rate)

    pair_rows = half + 2 * n_parts + pieces * width + 2 * pieces
    table = ((n_first + 2 * n_parts, LOW), BF)
    diffused0, sums0, slab_msg, pair0_msg, pair1_msg, stay_phi = call(
        functools.partial(first_kernel, n_grp, own),
        [
            (((depth + 2) * width, plane), F32),
            ((n_first + n_parts, LOW), F32),
            ((n_first + 2 * n_parts, LOW), BF),
            ((pair_rows, LOW), BF),
            ((pair_rows, LOW), BF),
            ((width, total), F32),
        ],
        [table, ((n_first + width, LOW), F32)],
        1 << 32,
    )(react, sorted_phi, codes, cells_f, weights, mine, *fields)

    received = []
    for shift in range(n_grp):
        if shift == 0:
            received.append(exchange(pair0_msg, "near", 0))
            received.append(exchange(pair1_msg, "far", 0))
        else:
            near = exchange(slab_msg, "near", shift)
            received += [exchange(near, "relay", shift), near]
            received.append(exchange(pair1_msg[: half + 2 * n_parts], "far", shift))

    n_own = 2 * n_parts * own
    outs = call(
        functools.partial(second_kernel, n_grp, own),
        [((width, total), F32), ((n_own + n_parts, LOW), F32), ((n_parts * own, LOW), F32)]
        + [((n_own + 2 * n_parts, LOW), BF)] * (n_grp - 1),
        [
            table,
            ((width, total), F32),
            ((1, total), jnp.int32),
            ((1, total), F32),
            (((depth + 2) * width, plane), F32),
            ((2 * n_first + width, LOW), F32),
        ],
        1 << 32,
    )(react, stay_phi, codes, weights, diffused0, sums0, *received)
    particles_out, own_sums, own_diffused = outs[:3]
    final = [exchange(outs[2 + shift], "same", shift) for shift in range(1, n_grp)]
    field_out, spread_out = call(
        functools.partial(last_kernel, n_grp, own),
        [(field.shape, F32), (field.shape, F32)],
        [],
        1 << 20,
        limit=8,
    )(own_sums, own_diffused, *final)
    return field_out, spread_out, particles_out


def solution(mesh):
    return jax.shard_map(
        shards,
        mesh=mesh,
        in_specs=(
            P("grp", "sp", None),
            P("sp", None),
            P(),
            P(None, ("grp", "sp")),
            P(None, ("grp", "sp")),
            P(("grp", "sp")),
            P(("grp", "sp")),
        ),
        out_specs=(P("grp", "sp", None), P("grp", "sp", None), P(None, ("grp", "sp"))),
        check_vma=False,
    )
```
